32 devices in a mesh: row: 4 (over x, core), theta: 4 (over z), phi: 2 (over y).
Axes of the slice: x: 2, y: 2, z: 4, core: 2. Of those that a mesh axis runs over, the one named last changes fastest.
Arguments:
- magnetic: float32 [3, 48, 64, 256], P(None, 'row', 'theta', 'phi'), may hold values from -6 to 6
- electric: float32 [3, 48, 64, 256], P(None, 'row', 'theta', 'phi'), may hold values from -6 to 6
Outputs:
- magnetic_new: float32 [3, 48, 64, 256], P(None, 'row', 'theta', 'phi')
- electric_new: float32 [3, 48, 64, 256], P(None, 'row', 'theta', 'phi')
The draws below stay inside these ranges and needn't reach their ends.
All inputs are finite; a program needn't handle non-finite values.
Results may differ from the reference program's by a relative error of at most 0.0001.
Values sent between devices are 32-bit elements; how exact they have to be, the bound alone decides.
No kernel may reach another device: no remote copies, remote signals or barrier semaphores. Data moves between devices by JAX's collectives and lax.ppermute only.
A program may use at most 64 MiB of HBM per device.

```python
import math
import jax
import jax.numpy as jnp
from jax import lax

NR = 48
NT = 64
NP = 256


def steps_of(rng, dims, pieces, smallest, high):
    def one(dim, shards_of):
        steps = jax.random.uniform(jax.random.fold_in(jax.random.fold_in(rng, 6), dim), (shards_of,), jnp.float32, smallest / len(pieces), high / len(pieces))
        return jnp.repeat(jnp.exp(steps), dims[dim] // shards_of).reshape((-1,) + (1,) * (len(dims) - dim - 1))

    loudness = one(*pieces[0])
    for cut in pieces[1:]:
        loudness = loudness * one(*cut)
    return loudness


def gaussian(own_key, extent, width, most, shards=(), kind=jnp.bfloat16):
    result = width * jax.random.normal(own_key, extent, jnp.float32)
    if shards:
        result = result * steps_of(own_key, extent, shards, -0.22, 0.18)
    return jnp.clip(result, -most, most).astype(kind)


def setup_inputs(seed: int = 0) -> dict:
    key_of = jax.random.split(jax.random.key(seed), 3)
    return {
        "magnetic": gaussian(key_of[0], (3, NR, NT, NP), 1.0, 6.0, ((1, 4), (2, 4), (3, 2)), jnp.float32),
        "electric": gaussian(key_of[1], (3, NR, NT, NP), 1.0, 6.0, ((1, 4), (2, 4), (3, 2)), jnp.float32),
    }


hole_mass = 1.0
inner_radius = 1.8
wave_speed = 1.25
courant = 0.3
smooth_eps = 1e-06

def weno_face(far_left, near_left, center, near_right, far_right):
    cand_low = (2.0 * far_left - 7.0 * near_left + 11.0 * center) / 6.0
    cand_mid = (-near_left + 5.0 * center + 2.0 * near_right) / 6.0
    cand_high = (2.0 * center + 5.0 * near_right - far_right) / 6.0
    rough_low = 13.0 / 12.0 * (far_left - 2.0 * near_left + center) ** 2 + 0.25 * (far_left - 4.0 * near_left + 3.0 * center) ** 2
    rough_mid = 13.0 / 12.0 * (near_left - 2.0 * center + near_right) ** 2 + 0.25 * (near_left - near_right) ** 2
    rough_high = 13.0 / 12.0 * (center - 2.0 * near_right + far_right) ** 2 + 0.25 * (3.0 * center - 4.0 * near_right + far_right) ** 2
    alpha_low = 0.1 / (smooth_eps + rough_low) ** 2
    alpha_mid = 0.6 / (smooth_eps + rough_mid) ** 2
    alpha_high = 0.3 / (smooth_eps + rough_high) ** 2
    return (alpha_low * cand_low + alpha_mid * cand_mid + alpha_high * cand_high) / (alpha_low + alpha_mid + alpha_high)

def interface(flux, field, axis):
    faces = flux.shape[axis] - 5
    plus_part = 0.5 * (flux + wave_speed * field)
    minus_part = 0.5 * (flux - wave_speed * field)
    plus_cuts = [lax.slice_in_dim(plus_part, offset, offset + faces, axis=axis) for offset in range(6)]
    minus_cuts = [lax.slice_in_dim(minus_part, offset, offset + faces, axis=axis) for offset in range(6)]
    left_state = weno_face(plus_cuts[0], plus_cuts[1], plus_cuts[2], plus_cuts[3], plus_cuts[4])
    right_state = weno_face(minus_cuts[5], minus_cuts[4], minus_cuts[3], minus_cuts[2], minus_cuts[1])
    return left_state + right_state

def face_fluxes(fluxes, fields, axis):
    return lax.map(lambda couple: interface(couple[0], couple[1], axis), (fluxes, fields))

def tendency(padded, radii, angles, spacing_r, spacing_theta, spacing_phi):
    ratio = 2.0 * hole_mass / radii
    lapse_factor = (1.0 / jnp.sqrt(1.0 + ratio))[:, None, None]
    shift_speed = (ratio / (1.0 + ratio))[:, None, None]
    b_radial, b_polar, b_azimuth = (padded[0], padded[1], padded[2])
    d_radial, d_polar, d_azimuth = (padded[3], padded[4], padded[5])
    e_radial = lapse_factor * d_radial
    e_polar = lapse_factor * d_polar - shift_speed * b_azimuth
    e_azimuth = lapse_factor * d_azimuth + shift_speed * b_polar
    h_radial = lapse_factor * b_radial
    h_polar = lapse_factor * b_polar + shift_speed * d_azimuth
    h_azimuth = lapse_factor * b_azimuth - shift_speed * d_polar
    zeros_field = jnp.zeros_like(b_radial)
    radial_flux = jnp.stack([zeros_field, -e_azimuth, e_polar, zeros_field, h_azimuth, -h_polar])
    polar_flux = jnp.stack([e_azimuth, zeros_field, -e_radial, -h_azimuth, zeros_field, h_radial])
    azimuth_flux = jnp.stack([-e_polar, e_radial, zeros_field, h_polar, -h_radial, zeros_field])
    radial_faces = face_fluxes(radial_flux[:, :, 3:-3, 3:-3], padded[:, :, 3:-3, 3:-3], 0)
    polar_faces = face_fluxes(polar_flux[:, 3:-3, :, 3:-3], padded[:, 3:-3, :, 3:-3], 1)
    azimuth_faces = face_fluxes(azimuth_flux[:, 3:-3, 3:-3, :], padded[:, 3:-3, 3:-3, :], 2)
    radius_face = (0.5 * (radii[2:-3] + radii[3:-2])) ** 2
    radius_cell = radii[3:-3] ** 2
    sine_face = jnp.sin(0.5 * (angles[2:-3] + angles[3:-2]))
    sine_cell = jnp.sin(angles[3:-3])
    radial_div = (radius_face[None, 1:, None, None] * radial_faces[:, 1:] - radius_face[None, :-1, None, None] * radial_faces[:, :-1]) / (radius_cell[None, :, None, None] * spacing_r)
    polar_div = (sine_face[None, None, 1:, None] * polar_faces[:, :, 1:] - sine_face[None, None, :-1, None] * polar_faces[:, :, :-1]) / (sine_cell[None, None, :, None] * spacing_theta)
    azimuth_div = (azimuth_faces[:, :, :, 1:] - azimuth_faces[:, :, :, :-1]) / spacing_phi
    return -(radial_div + polar_div + azimuth_div)

def project(fields):
    magnetic_part = fields[:3]
    electric_part = fields[3:]
    b_square = jnp.maximum(lax.optimization_barrier(jnp.sum(magnetic_part * magnetic_part, axis=0)), 1.0)
    along = lax.optimization_barrier(jnp.sum(magnetic_part * electric_part, axis=0)) / b_square
    electric_part = electric_part - along[None] * magnetic_part
    d_square = lax.optimization_barrier(jnp.sum(electric_part * electric_part, axis=0))
    shrink = jnp.sqrt(b_square / jnp.maximum(d_square, b_square))
    return jnp.concatenate([magnetic_part, electric_part * shrink[None]], axis=0)

def extend(fields):
    grown = jnp.pad(fields, ((0, 0), (3, 3), (0, 0), (0, 0)))
    parity = jnp.array([1.0, -1.0, -1.0, 1.0, -1.0, -1.0], jnp.float32)[:, None, None, None]
    half_turn = grown.shape[3] // 2
    north_rows = jnp.roll(grown[:, :, 2::-1, :], half_turn, axis=3) * parity
    south_rows = jnp.roll(grown[:, :, :-4:-1, :], half_turn, axis=3) * parity
    grown = jnp.concatenate([north_rows, grown, south_rows], axis=2)
    return jnp.concatenate([grown[..., -3:], grown, grown[..., :3]], axis=3)

def reference(magnetic, electric):
    fields = jnp.concatenate([magnetic, electric], axis=0)
    spacing_theta = math.pi / NT
    spacing_r = spacing_theta
    spacing_phi = 2.0 * math.pi / NP
    step_dt = courant / (1.0 / spacing_r + 1.0 / spacing_theta + 1.0 / spacing_phi)
    radii = inner_radius + (jnp.arange(-3, NR + 3).astype(jnp.float32) + 0.5) * spacing_r
    angles = (jnp.arange(-3, NT + 3).astype(jnp.float32) + 0.5) * spacing_theta
    current = fields
    for weight in (0.0, 0.75, 1.0 / 3.0):
        rates = tendency(extend(current), radii, angles, spacing_r, spacing_theta, spacing_phi)
        current = project(weight * fields + (1.0 - weight) * (current + step_dt * rates))
    return (current[:3], current[3:])
```

```python
import functools
import math

import jax
import jax.numpy as jnp
from jax import lax
from jax.experimental import pallas as pl
from jax.experimental.pallas import tpu as pltpu
from jax.sharding import PartitionSpec as P

hole_mass = 1.0
inner_radius = 1.8
wave_speed = 1.25
courant = 0.3
smooth_eps = 1e-06

G = 3
HALF = 0.5 * wave_speed
EPS = smooth_eps / (HALF * HALF)

B1, B3, D1, D3, B2, D2 = range(6)
E3, NE1, NH3, H1, E2, NH2 = range(6)
FROM_ARGS = ((0, 0), (0, 2), (1, 0), (1, 2), (0, 1), (1, 1))
RADIAL = {B1: None, B3: (E2, 1), D1: None, D3: (NH2, 1), B2: (E3, -1), D2: (NH3, -1)}
PHI_U = (B1, B2, D1, D2, B3, D3)
PHI_E = (E2, NE1, NH2, H1)
PARITY = {B1: 1.0, B3: -1.0, D1: 1.0, D3: -1.0, B2: -1.0, D2: -1.0}


class Lazy:
    def __init__(self, make):
        self.make, self.kept = make, {}

    def __call__(self, k):
        if k not in self.kept:
            self.kept[k] = self.make(k)
        return self.kept[k]


class Rough:
    def __init__(self, value):
        self.diff = Lazy(lambda k: value(k + 1) - value(k))
        self.second = Lazy(lambda k: self.diff(k) - self.diff(k - 1))
        self.third = Lazy(lambda k: self.second(k + 1) - self.second(k))
        self.twice = Lazy(lambda k: self.second(k) + self.second(k))
        self.mid = Lazy(
            lambda k: (self.twice(k) * self.twice(k)) * (1.0 / 3.0)
            + (self.diff(k) * self.diff(k - 1) + EPS)
        )
        self.sq_low = Lazy(lambda k: square(self.mid(k) + self.diff(k) * self.twice(k)))
        self.sq_mid = Lazy(lambda k: square(self.mid(k)))
        self.sq_high = Lazy(lambda k: square(self.mid(k) - self.diff(k - 1) * self.twice(k)))


def square(x):
    return x * x


def correction(outer, mid, inner, third_outer, third_mid):
    outer3 = 3.0 * outer
    inner2 = inner + inner
    top = mid * (inner2 * third_outer + outer3 * third_mid)
    bottom = mid * (inner + outer3) + outer3 * inner2
    return top / bottom


def walk(faces, get_u, get_e, sign, emit):
    u = Lazy(get_u)
    if get_e is None:
        plus = minus = Rough(u)
    else:
        e = Lazy(get_e)
        total = Lazy(lambda k: e(k) + u(k))
        gap = Lazy(lambda k: e(k) - u(k))
        plus, minus = (Rough(total), Rough(gap)) if sign > 0 else (Rough(gap), Rough(total))
    previous = None
    for f in range(faces):
        i = f + 2
        left = correction(
            plus.sq_low(i - 1), plus.sq_mid(i), plus.sq_high(i + 1),
            plus.third(i - 1), plus.third(i),
        )
        right = correction(
            minus.sq_high(i + 2), minus.sq_mid(i + 1), minus.sq_low(i),
            minus.third(i + 1), minus.third(i),
        )
        if get_e is None:
            flux = (plus.third(i) - left) - right
        else:
            flux = (
                (7.0 * (e(i) + e(i + 1)) - (e(i - 1) + e(i + 2)))
                + 0.5 * (plus.third(i) - minus.third(i))
            ) + (right - left)
        if f:
            emit(f - 1, previous, flux)
        previous = flux


def fields_of(c, a, s):
    return (
        a * c[D3] + s * c[B2],
        -(a * c[D1]),
        s * c[D2] - a * c[B3],
        a * c[B1],
        a * c[D2] - s * c[B3],
        -(a * c[B2] + s * c[D3]),
    )


class Sizes:
    def __init__(self, rows, thetas, phis):
        self.R, self.T, self.L = rows, thetas, phis
        self.slices = 6 * rows
        self.per = self.L // self.T
        self.n_u = self.slices // self.per
        self.n_e = 4 * rows // self.per
        self.n_t = self.n_u + self.n_e
        self.step = self.L // 8
        self.k_a = 0
        self.k_s = rows + 2 * G
        self.k_rp = 2 * self.k_s
        self.k_rm = self.k_rp + rows
        self.k_tp = self.k_rm + rows
        self.k_tm = self.k_tp + thetas
        self.k_par = -(-(self.k_tm + thetas) // 8) * 8
        self.k_n = self.k_par + self.slices

    def check(self):
        assert self.T % 8 == 0 and self.L % self.T == 0 and self.L == 128
        assert (4 * self.R) % 8 == 0 and (2 * self.R) % 8 == 0
        assert (4 * self.R) % self.per == 0 and (2 * self.R) % self.per == 0


def prep(z, scal, co, u_ref, e_ref, pt_ref, ra_ref, rb_ref, ta_ref, tb_ref, p_ref):
    R, T, L = z.R, z.T, z.L

    def fields_at(r, carry):
        a = co[pl.ds(z.k_a + G + r, 1), :]
        s = co[pl.ds(z.k_s + G + r, 1), :]
        for t in range(0, T, 8):
            row = pl.multiple_of(r * T + t, 8)
            c = [u_ref[pl.ds(k * R * T + row, 8), :] for k in range(6)]
            for k, value in enumerate(fields_of(c, a, s)):
                e_ref[pl.ds(k * R * T + row, 8), :] = value
        return carry

    lax.fori_loop(0, R, fields_at, 0, unroll=2)

    def turned(ref, comps, block):
        parts = []
        for n in range(block * z.per, (block + 1) * z.per):
            row = (comps[n // R] * R + n % R) * T
            parts.append(ref[row : row + T, :])
        return jnp.concatenate(parts, axis=0).T

    for b in range(z.n_u):
        pt_ref[b] = turned(u_ref, PHI_U, b)
    for b in range(z.n_e):
        pt_ref[z.n_u + b] = turned(e_ref, PHI_E, b)
    flat = pt_ref.reshape(z.n_t * L, L)
    for k in range(G):
        for n in range(0, z.n_t, 8):
            m = min(8, z.n_t - n)
            p_ref[k, n : n + m, :] = flat[pl.ds(n * L + k, m, stride=L), :]
            p_ref[G + k, n : n + m, :] = flat[pl.ds(n * L + L - G + k, m, stride=L), :]

    def rows_to(ref, start):
        for c in range(6):
            ref[c * G * T : (c + 1) * G * T, :] = u_ref[
                (c * R + start) * T : (c * R + start + G) * T, :
            ]

    def polar_to(ref, picks, flip):
        for k, pick in enumerate(picks):
            for n in range(0, z.slices, 8):
                value = u_ref[pl.ds(n * T + pick, 8, stride=T), :]
                if flip:
                    value = value * co[z.k_par + n : z.k_par + n + 8, :]
                ref[k * z.slices + n : k * z.slices + n + 8, :] = value

    row_even, theta_even, north, south = scal[0] == 1, scal[1] == 1, scal[2] == 1, scal[3] == 1

    def low_polar(ref):
        pl.when(north)(lambda: polar_to(ref, (2, 1, 0), True))
        pl.when(jnp.logical_not(north))(lambda: polar_to(ref, (0, 1, 2), False))

    def high_polar(ref):
        pl.when(south)(lambda: polar_to(ref, (T - 1, T - 2, T - 3), True))
        pl.when(jnp.logical_not(south))(lambda: polar_to(ref, (T - 3, T - 2, T - 1), False))

    @pl.when(row_even)
    def _():
        rows_to(ra_ref, R - G)
        rows_to(rb_ref, 0)

    @pl.when(jnp.logical_not(row_even))
    def _():
        rows_to(ra_ref, 0)
        rows_to(rb_ref, R - G)

    @pl.when(theta_even)
    def _():
        low_polar(ta_ref)
        high_polar(tb_ref)

    @pl.when(jnp.logical_not(theta_even))
    def _():
        low_polar(tb_ref)
        high_polar(ta_ref)


def first_kernel(z, scal, co, m_ref, d_ref, *outs):
    u_ref = outs[0]
    n = z.R * z.T
    for c, (which, k) in enumerate(FROM_ARGS):
        u_ref[c * n : (c + 1) * n, :] = (m_ref, d_ref)[which][k * n : (k + 1) * n, :]
    prep(z, scal, co, *outs)


def stage_kernel(z, weight, last, step_phi, *refs):
    refs = list(refs)
    scal, co, u_ref, e_ref, pt_ref, ra, rb, ta, tb, pr = refs[:10]
    refs = refs[10:]
    u0_ref = None
    if weight:
        u0_ref = refs.pop(0)
    if last:
        m_ref, d_ref = refs[:2]
        refs = refs[2:]
    else:
        outs = refs[:8]
        refs = refs[8:]
    new, pad, turned, acc_p, acc_t, rows_u, rows_e, pol_u, pol_e = refs
    R, T, L = z.R, z.T, z.L
    row_even, theta_even = scal[0] == 1, scal[1] == 1

    def pad_block(b, carry):
        pad[b, 8 : 8 + L, :] = pt_ref[b]
        return carry

    lax.fori_loop(0, z.n_t, pad_block, 0)
    tall = L + 16
    flat = pad.reshape(z.n_t * tall, L)
    for k in range(G):
        for n in range(0, z.n_t, 8):
            m = min(8, z.n_t - n)
            flat[pl.ds(n * tall + 8 + L + k, m, stride=tall), :] = pr[k, n : n + m, :]
            flat[pl.ds(n * tall + 8 - G + k, m, stride=tall), :] = pr[G + k, n : n + m, :]

    def phi_block(b, carry, has_e):
        def at(block):
            return lambda k: pad[block, pl.ds(8 - G + k, 8, stride=z.step), :]

        scale = -step_phi if has_e else step_phi

        def emit(j, low, high):
            turned[pl.ds(j, 8, stride=z.step), :] = scale * (high - low)

        walk(z.step + 1, at(b), at(z.n_u + b) if has_e else None, -1, emit)
        acc_p[pl.ds(pl.multiple_of(b * L, L), L), :] = turned[...].T
        return carry

    lax.fori_loop(0, z.n_e, functools.partial(phi_block, has_e=True), 0)
    lax.fori_loop(z.n_e, z.n_u, functools.partial(phi_block, has_e=False), 0)

    def polar_in(low, high):
        pol_u[0 : G * z.slices, :] = low[...]
        pol_u[G * z.slices :, :] = high[...]

    pl.when(theta_even)(lambda: polar_in(ta, tb))
    pl.when(jnp.logical_not(theta_even))(lambda: polar_in(tb, ta))
    for k in range(2 * G):
        c = [pol_u[k * z.slices + n * R : k * z.slices + (n + 1) * R, :] for n in range(6)]
        a = co[z.k_a + G : z.k_a + G + R, :]
        s = co[z.k_s + G : z.k_s + G + R, :]
        for n, value in enumerate(fields_of(c, a, s)[:4]):
            pol_e[(k * 4 + n) * R : (k * 4 + n + 1) * R, :] = value

    def theta_group(g, carry, has_e):
        def at(ref, ghosts, per):
            def get(k):
                if G <= k < G + T:
                    return ref[pl.ds(g * 8 * T + (k - G), 8, stride=T), :]
                ghost = k if k < G else k - T
                return ghosts[pl.ds(pl.multiple_of(ghost * per + g * 8, 8), 8), :]

            return get

        def emit(j, low, high):
            acc_t[pl.ds(g * 8 * T + j, 8, stride=T), :] = (
                co[z.k_tp + j : z.k_tp + j + 1, :] * high
                - co[z.k_tm + j : z.k_tm + j + 1, :] * low
            )

        get_e = at(e_ref, pol_e, 4 * R) if has_e else None
        walk(T + 1, at(u_ref, pol_u, z.slices), get_e, 1, emit)
        return carry

    lax.fori_loop(0, 4 * R // 8, functools.partial(theta_group, has_e=True), 0)
    lax.fori_loop(4 * R // 8, z.slices // 8, functools.partial(theta_group, has_e=False), 0)

    def rows_in(low, high):
        for c in range(6):
            span = slice(c * G * T, (c + 1) * G * T)
            rows_u[2 * c * G * T : (2 * c + 1) * G * T, :] = low[span, :]
            rows_u[(2 * c + 1) * G * T : (2 * c + 2) * G * T, :] = high[span, :]

    pl.when(row_even)(lambda: rows_in(rb, ra))
    pl.when(jnp.logical_not(row_even))(lambda: rows_in(ra, rb))
    for k in range(2 * G):
        r = k if k < G else k + R
        a = co[z.k_a + r : z.k_a + r + 1, :]
        s = co[z.k_s + r : z.k_s + r + 1, :]
        for t in range(0, T, 8):
            c = [rows_u[(2 * G * n + k) * T + t : (2 * G * n + k) * T + t + 8, :] for n in range(6)]
            values = fields_of(c, a, s)
            for n in (E3, NH3, E2, NH2):
                rows_e[(2 * G * n + k) * T + t : (2 * G * n + k) * T + t + 8, :] = values[n]

    def radial_tile(t, carry):
        base = pl.multiple_of(t * 8, 8)
        for c in range(6):
            def at(ref, ghosts, n):
                def get(k):
                    if G <= k < G + R:
                        return ref[pl.ds((n * R + k - G) * T + base, 8), :]
                    ghost = k if k < G else k - R
                    return ghosts[pl.ds((2 * G * n + ghost) * T + base, 8), :]

                return get

            spec = RADIAL[c]
            sign = spec[1] if spec else 1

            def emit(j, low, high):
                row = (c * R + j) * T + base
                across = (PHI_U.index(c) * R + j) * T + base
                inc = (
                    co[z.k_rp + j : z.k_rp + j + 1, :] * high
                    - co[z.k_rm + j : z.k_rm + j + 1, :] * low
                )
                rest = acc_t[pl.ds(row, 8), :] + acc_p[pl.ds(across, 8), :]
                inc = rest + inc if sign > 0 else rest - inc
                value = u_ref[pl.ds(row, 8), :] + inc
                if weight:
                    value = (1.0 - weight) * value + weight * u0_ref[pl.ds(row, 8), :]
                new[pl.ds(row, 8), :] = value

            get_e = at(e_ref, rows_e, spec[0]) if spec else None
            walk(R + 1, at(u_ref, rows_u, c), get_e, sign, emit)
        return carry

    lax.fori_loop(0, T // 8, radial_tile, 0)

    n = R * T

    def project(i, carry):
        row = pl.multiple_of(i * 8, 8)
        c = [new[pl.ds(k * n + row, 8), :] for k in range(6)]
        b = (c[B1], c[B2], c[B3])
        d = (c[D1], c[D2], c[D3])
        b_square = jnp.maximum(b[0] * b[0] + b[1] * b[1] + b[2] * b[2], 1.0)
        along = (b[0] * d[0] + b[1] * d[1] + b[2] * d[2]) / b_square
        d = [dk - along * bk for dk, bk in zip(d, b)]
        d_square = d[0] * d[0] + d[1] * d[1] + d[2] * d[2]
        shrink = jnp.sqrt(b_square / jnp.maximum(d_square, b_square))
        d = [dk * shrink for dk in d]
        if last:
            for k in range(3):
                m_ref[pl.ds(k * n + row, 8), :] = b[k]
                d_ref[pl.ds(k * n + row, 8), :] = d[k]
        else:
            for k, value in zip((B1, B2, B3, D1, D2, D3), (*b, *d)):
                outs[0][pl.ds(k * n + row, 8), :] = value
        return carry

    lax.fori_loop(0, n // 8, project, 0, unroll=4)
    if not last:
        prep(z, scal, co, *outs)


def body(mesh, magnetic, electric):
    n_row, n_theta, n_phi = (mesh.shape[k] for k in ("row", "theta", "phi"))
    _, R, T, L = magnetic.shape
    z = Sizes(R, T, L)
    z.check()
    f32 = jnp.float32
    d_theta = math.pi / (T * n_theta)
    d_phi = 2.0 * math.pi / (L * n_phi)
    step_dt = courant / (2.0 / d_theta + 1.0 / d_phi)
    unit = -step_dt * HALF / 6.0

    i_row, i_theta = lax.axis_index("row"), lax.axis_index("theta")
    scal = jnp.stack(
        [(i_row % 2 == 0), (i_theta % 2 == 0), (i_theta == 0), (i_theta == n_theta - 1)]
    ).astype(jnp.int32)
    radii = inner_radius + ((i_row * R - G + jnp.arange(R + 2 * G)).astype(f32) + 0.5) * d_theta
    angles = ((i_theta * T - G + jnp.arange(T + 2 * G)).astype(f32) + 0.5) * d_theta
    ratio = 2.0 * hole_mass / radii
    lapse = 1.0 / jnp.sqrt(1.0 + ratio) / wave_speed
    shift = ratio / (1.0 + ratio) / wave_speed
    r_face = (0.5 * (radii[G - 1 : -G] + radii[G : 1 - G])) ** 2
    r_scale = unit / (radii[G:-G] ** 2 * d_theta)
    t_face = jnp.sin(0.5 * (angles[G - 1 : -G] + angles[G : 1 - G]))
    t_scale = unit / (jnp.sin(angles[G:-G]) * d_theta)
    parity = jnp.repeat(jnp.array([PARITY[c] for c in range(6)], f32), R)
    parts = [
        lapse, shift, r_face[1:] * r_scale, r_face[:-1] * r_scale,
        t_face[1:] * t_scale, t_face[:-1] * t_scale,
    ]
    used = sum(p.shape[0] for p in parts)
    table = jnp.concatenate(parts + [jnp.zeros((z.k_par - used,), f32), parity])
    co = jnp.broadcast_to(table[:, None], (z.k_n, L))

    vmem = pl.BlockSpec(memory_space=pltpu.VMEM)
    smem = pl.BlockSpec(memory_space=pltpu.SMEM)
    whole = (z.slices * T, L)
    state_shapes = [
        whole, whole, (z.n_t, L, L),
        (6 * G * T, L), (6 * G * T, L), (G * z.slices, L), (G * z.slices, L), (2 * G, z.n_t, L),
    ]
    state_out = [jax.ShapeDtypeStruct(s, f32) for s in state_shapes]
    half_out = [jax.ShapeDtypeStruct((3 * R * T, L), f32)] * 2
    scratch = [
        pltpu.VMEM(whole, f32),
        pltpu.VMEM((z.n_t, L + 16, L), f32),
        pltpu.VMEM((L, L), f32),
        pltpu.VMEM(whole, f32),
        pltpu.VMEM(whole, f32),
        pltpu.VMEM((6 * 2 * G * T, L), f32),
        pltpu.VMEM((6 * 2 * G * T, L), f32),
        pltpu.VMEM((2 * G * z.slices, L), f32),
        pltpu.VMEM((2 * G * 4 * R, L), f32),
    ]

    row_a = [p for k in range(0, n_row - 1, 2) for p in ((k, k + 1), (k + 1, k))]
    row_b = [p for k in range(1, n_row - 1, 2) for p in ((k, k + 1), (k + 1, k))]

    def polar_pairs(odd):
        pairs = []
        for k in range(-1, n_theta):
            if k % 2 != odd:
                continue
            for p in range(n_phi):
                if k in (-1, n_theta - 1):
                    t = max(k, 0)
                    pairs.append((t * n_phi + p, t * n_phi + (p + n_phi // 2) % n_phi))
                else:
                    low, high = k * n_phi + p, (k + 1) * n_phi + p
                    pairs += [(low, high), (high, low)]
        return pairs

    def exchange(ra, rb, ta, tb, p):
        left = [(k, (k - 1) % n_phi) for k in range(n_phi)]
        right = [(k, (k + 1) % n_phi) for k in range(n_phi)]
        if n_phi == 2:
            p = lax.ppermute(p, "phi", left)
        else:
            p = jnp.concatenate(
                [lax.ppermute(p[:G], "phi", left), lax.ppermute(p[G:], "phi", right)]
            )
        return (
            lax.ppermute(ra, "row", row_a),
            lax.ppermute(rb, "row", row_b),
            lax.ppermute(ta, ("theta", "phi"), polar_pairs(1)),
            lax.ppermute(tb, ("theta", "phi"), polar_pairs(0)),
            p,
        )

    state = pl.pallas_call(
        functools.partial(first_kernel, z),
        out_shape=state_out,
        in_specs=[smem, vmem, vmem, vmem],
        out_specs=[vmem] * 8,
        name="first",
    )(scal, co, magnetic.reshape(-1, L), electric.reshape(-1, L))
    start = state[0]
    weights = (0.0, 0.75, 1.0 / 3.0)
    for n, weight in enumerate(weights):
        last = n == len(weights) - 1
        extra = [start] if weight else []
        state = pl.pallas_call(
            functools.partial(stage_kernel, z, weight, last, unit / d_phi),
            out_shape=half_out if last else state_out,
            in_specs=[smem] + [vmem] * (9 + len(extra)),
            out_specs=[vmem] * (2 if last else 8),
            scratch_shapes=scratch,
            name=f"stage{n}",
        )(scal, co, *state[:3], *exchange(*state[3:]), *extra)
    return tuple(s.reshape(magnetic.shape) for s in state)


def solution(mesh):
    spec = P(None, "row", "theta", "phi")
    return jax.shard_map(
        functools.partial(body, mesh),
        mesh=mesh, in_specs=(spec, spec), out_specs=(spec, spec), check_vma=False,
    )
```

```python
import functools
import math

import jax
import jax.numpy as jnp
from jax import lax
from jax.experimental import pallas as pl
from jax.experimental.pallas import tpu as pltpu
from jax.sharding import PartitionSpec as P

hole_mass = 1.0
inner_radius = 1.8
wave_speed = 1.25
courant = 0.3
smooth_eps = 1e-06

G = 3
VMEM_LIMIT = 24 * 2**20
HALF = 0.5 * wave_speed
EPS = smooth_eps / (HALF * HALF)

B1, B3, D1, D3, B2, D2 = range(6)
E3, NE1, NH3, H1, E2, NH2 = range(6)
FROM_ARGS = ((0, 0), (0, 2), (1, 0), (1, 2), (0, 1), (1, 1))
RADIAL = {B1: None, B3: (E2, 1), D1: None, D3: (NH2, 1), B2: (E3, -1), D2: (NH3, -1)}
PHI_U = (B1, B2, D1, D2, B3, D3)
PHI_E = (E2, NE1, NH2, H1)
PARITY = {B1: 1.0, B3: -1.0, D1: 1.0, D3: -1.0, B2: -1.0, D2: -1.0}


class Lazy:
    def __init__(self, make):
        self.make, self.kept = make, {}

    def __call__(self, k):
        if k not in self.kept:
            self.kept[k] = self.make(k)
        return self.kept[k]


class Rough:
    def __init__(self, value):
        self.diff = Lazy(lambda k: value(k + 1) - value(k))
        self.second = Lazy(lambda k: self.diff(k) - self.diff(k - 1))
        self.third = Lazy(lambda k: self.second(k + 1) - self.second(k))
        self.twice = Lazy(lambda k: self.second(k) + self.second(k))
        self.mid = Lazy(
            lambda k: (self.twice(k) * self.twice(k)) * (1.0 / 3.0)
            + (self.diff(k) * self.diff(k - 1) + EPS)
        )
        self.sq_low = Lazy(lambda k: square(self.mid(k) + self.diff(k) * self.twice(k)))
        self.sq_mid = Lazy(lambda k: square(self.mid(k)))
        self.sq_high = Lazy(lambda k: square(self.mid(k) - self.diff(k - 1) * self.twice(k)))


def square(x):
    return x * x


def correction(outer, mid, inner, third_outer, third_mid):
    outer3 = 3.0 * outer
    inner2 = inner + inner
    top = mid * (inner2 * third_outer + outer3 * third_mid)
    bottom = mid * (inner + outer3) + outer3 * inner2
    return top / bottom


def walk(faces, get_u, get_e, sign, emit):
    u = Lazy(get_u)
    if get_e is None:
        plus = minus = Rough(u)
    else:
        e = Lazy(get_e)
        total = Lazy(lambda k: e(k) + u(k))
        gap = Lazy(lambda k: e(k) - u(k))
        plus, minus = (Rough(total), Rough(gap)) if sign > 0 else (Rough(gap), Rough(total))
    previous = None
    for f in range(faces):
        i = f + 2
        left = correction(
            plus.sq_low(i - 1), plus.sq_mid(i), plus.sq_high(i + 1),
            plus.third(i - 1), plus.third(i),
        )
        right = correction(
            minus.sq_high(i + 2), minus.sq_mid(i + 1), minus.sq_low(i),
            minus.third(i + 1), minus.third(i),
        )
        if get_e is None:
            flux = (plus.third(i) - left) - right
        else:
            flux = (
                (7.0 * (e(i) + e(i + 1)) - (e(i - 1) + e(i + 2)))
                + 0.5 * (plus.third(i) - minus.third(i))
            ) + (right - left)
        if f:
            emit(f - 1, previous, flux)
        previous = flux


def fields_of(c, a, s):
    return (
        a * c[D3] + s * c[B2],
        -(a * c[D1]),
        s * c[D2] - a * c[B3],
        a * c[B1],
        a * c[D2] - s * c[B3],
        -(a * c[B2] + s * c[D3]),
    )


class Sizes:
    def __init__(self, mesh, rows, thetas, phis):
        self.n_row, self.n_theta, self.n_phi = (mesh.shape[k] for k in ("row", "theta", "phi"))
        self.R, self.T, self.L = rows, thetas, phis
        self.slices = 6 * rows
        self.per = self.L // self.T
        self.n_u = self.slices // self.per
        self.n_e = 4 * rows // self.per
        self.n_t = self.n_u + self.n_e
        self.step = self.L // 8
        self.d_theta = math.pi / (thetas * self.n_theta)
        self.d_phi = 2.0 * math.pi / (phis * self.n_phi)
        step_dt = courant / (2.0 / self.d_theta + 1.0 / self.d_phi)
        self.unit = -step_dt * HALF / 6.0
        at = 0
        for name, count in (
            ("k_a", rows + 2 * G), ("k_s", rows + 2 * G), ("k_rp", rows), ("k_rm", rows),
            ("k_tp", thetas), ("k_tm", thetas), ("k_par", self.slices),
        ):
            setattr(self, name, at)
            at += -(-count // 8) * 8
        self.k_n = at

    def check(self):
        assert self.T % 8 == 0 and self.L % self.T == 0 and self.L == 128
        assert self.T == self.step
        assert (4 * self.R) % 8 == 0 and (2 * self.R) % 8 == 0
        assert (4 * self.R) % self.per == 0 and (2 * self.R) % self.per == 0


def table(z, co):
    R, T, L = z.R, z.T, z.L
    f32 = jnp.float32

    def rows(count):
        return lax.broadcasted_iota(jnp.int32, (-(-count // 8) * 8, L), 0)

    def radius(count, first):
        row = rows(count) + (lax.axis_index("row") * R + first)
        return inner_radius + (row.astype(f32) + 0.5) * z.d_theta

    def angle(count, first):
        row = rows(count) + (lax.axis_index("theta") * T + first)
        return (row.astype(f32) + 0.5) * z.d_theta

    def put(at, value):
        co[at : at + value.shape[0], :] = value

    ratio = 2.0 * hole_mass / radius(R + 2 * G, -G)
    put(z.k_a, 1.0 / jnp.sqrt(1.0 + ratio) / wave_speed)
    put(z.k_s, ratio / (1.0 + ratio) / wave_speed)
    low, mid, high = (radius(R, k) for k in (-1, 0, 1))
    scale = z.unit / (mid * mid * z.d_theta)
    put(z.k_rp, square(0.5 * (mid + high)) * scale)
    put(z.k_rm, square(0.5 * (low + mid)) * scale)
    low, mid, high = (angle(T, k) for k in (-1, 0, 1))
    scale = z.unit / (jnp.sin(mid) * z.d_theta)
    put(z.k_tp, jnp.sin(0.5 * (mid + high)) * scale)
    put(z.k_tm, jnp.sin(0.5 * (low + mid)) * scale)
    for c in range(6):
        co[z.k_par + c * R : z.k_par + (c + 1) * R, :] = jnp.full((R, L), PARITY[c], f32)


RADIAL_E = (E3, NH3, E2, NH2)


def conditions(z):
    row, theta = lax.axis_index("row"), lax.axis_index("theta")
    return row % 2 == 0, theta % 2 == 0, theta == 0, theta == z.n_theta - 1


def prep(z, co, u_ref, e_ref, ut_ref, et_ref, pt_ref, ra_ref, rb_ref, ta_ref, tb_ref, p_ref, nat):
    R, T, L = z.R, z.T, z.L

    def fields_at(r, carry):
        a = co[pl.ds(z.k_a + G + r, 1), :]
        s = co[pl.ds(z.k_s + G + r, 1), :]
        for t in range(0, T, 8):
            row = pl.multiple_of(r * T + t, 8)
            c = [u_ref[pl.ds(k * R * T + row, 8), :] for k in range(6)]
            values = fields_of(c, a, s)
            for n, k in enumerate(RADIAL_E):
                e_ref[pl.ds(n * R * T + row, 8), :] = values[k]
            for n, k in enumerate(PHI_E):
                nat[pl.ds(n * R * T + row, 8), :] = values[k]
            for k in range(6):
                ut_ref[pl.ds(t * z.slices + k * R + r, 8, stride=z.slices), :] = c[k]
            for k in range(4):
                et_ref[pl.ds(t * 4 * R + k * R + r, 8, stride=4 * R), :] = values[k]
        return carry

    lax.fori_loop(0, R, fields_at, 0, unroll=2)

    def turn(ref, comps, block, into):
        parts = []
        for n in range(block * z.per, (block + 1) * z.per):
            row = (comps[n // R] * R + n % R) * T
            parts.append(ref[row : row + T, :])
        value = jnp.concatenate(parts, axis=0).T
        for n in range(0, L, 8):
            pt_ref[into, pl.ds((n % z.step) * 8 + n // z.step, 8, stride=8), :] = value[n : n + 8]

    for b in range(z.n_u):
        turn(u_ref, PHI_U, b, b)
    for b in range(z.n_e):
        turn(nat, range(4), b, z.n_u + b)
    for b in range(z.n_t):
        for k in range(G):
            p_ref[k, b : b + 1, :] = pt_ref[b, 8 * k : 8 * k + 1, :]
            row = 8 * (z.step - G + k) + 7
            p_ref[G + k, b : b + 1, :] = pt_ref[b, row : row + 1, :]

    def rows_to(ref, start):
        for c in range(6):
            ref[c * G * T : (c + 1) * G * T, :] = u_ref[
                (c * R + start) * T : (c * R + start + G) * T, :
            ]

    def polar_to(ref, picks, flip):
        parity = co[z.k_par : z.k_par + z.slices, :] if flip else None
        for k, pick in enumerate(picks):
            value = ut_ref[pick * z.slices : (pick + 1) * z.slices, :]
            ref[k * z.slices : (k + 1) * z.slices, :] = value * parity if flip else value

    row_even, theta_even, north, south = conditions(z)

    def low_polar(ref):
        pl.when(north)(lambda: polar_to(ref, (2, 1, 0), True))
        pl.when(jnp.logical_not(north))(lambda: polar_to(ref, (0, 1, 2), False))

    def high_polar(ref):
        pl.when(south)(lambda: polar_to(ref, (T - 1, T - 2, T - 3), True))
        pl.when(jnp.logical_not(south))(lambda: polar_to(ref, (T - 3, T - 2, T - 1), False))

    @pl.when(row_even)
    def _():
        rows_to(ra_ref, R - G)
        rows_to(rb_ref, 0)

    @pl.when(jnp.logical_not(row_even))
    def _():
        rows_to(ra_ref, 0)
        rows_to(rb_ref, R - G)

    @pl.when(theta_even)
    def _():
        low_polar(ta_ref)
        high_polar(tb_ref)

    @pl.when(jnp.logical_not(theta_even))
    def _():
        low_polar(tb_ref)
        high_polar(ta_ref)


def first_kernel(z, m_ref, d_ref, co, *rest):
    table(z, co)
    u_ref = rest[0]
    n = z.R * z.T
    for c, (which, k) in enumerate(FROM_ARGS):
        u_ref[c * n : (c + 1) * n, :] = (m_ref, d_ref)[which][k * n : (k + 1) * n, :]
    prep(z, co, *rest)


def stage_kernel(z, weight, last, *refs):
    refs = list(refs)
    co, u_ref, e_ref, ut, et, pt, ra, rb, ta, tb, pr = refs[:11]
    refs = refs[11:]
    u0_ref = None
    if weight:
        u0_ref = refs.pop(0)
    if last:
        m_ref, d_ref = refs[:2]
        refs = refs[2:]
    else:
        outs = refs[:10]
        refs = refs[10:]
    new, turned, acc_p, acc_t, rows_u, rows_e, pol_u, pol_e = refs
    R, T, L = z.R, z.T, z.L
    row_even, theta_even, _, _ = conditions(z)

    lane_row = lax.broadcasted_iota(jnp.int32, (8, L), 0)

    def phi_block(b, carry, has_e):
        def at(block):
            def get(k):
                cell = k - G
                wrapped = cell % z.step
                value = pt[block, 8 * wrapped : 8 * wrapped + 8, :]
                if cell < 0:
                    ghost = pr[G + k, pl.ds(block, 1), :]
                    value = jnp.where(lane_row == 0, ghost, pltpu.roll(value, 1, 0))
                elif cell >= z.step:
                    ghost = pr[cell - z.step, pl.ds(block, 1), :]
                    value = jnp.where(lane_row == 7, ghost, pltpu.roll(value, 7, 0))
                return value

            return get

        scale = -z.unit / z.d_phi if has_e else z.unit / z.d_phi

        def emit(j, low, high):
            turned[b, 8 * j : 8 * j + 8, :] = scale * (high - low)

        walk(z.step + 1, at(b), at(z.n_u + b) if has_e else None, -1, emit)
        return carry

    lax.fori_loop(0, z.n_e, functools.partial(phi_block, has_e=True), 0)
    lax.fori_loop(z.n_e, z.n_u, functools.partial(phi_block, has_e=False), 0)
    for b in range(z.n_u):
        parts = [
            turned[b, pl.ds((n % z.step) * 8 + n // z.step, 8, stride=8), :]
            for n in range(0, L, 8)
        ]
        acc_p[b * L : (b + 1) * L, :] = jnp.concatenate(parts, axis=0).T

    def polar_in(low, high):
        pol_u[0 : G * z.slices, :] = low[...]
        pol_u[G * z.slices :, :] = high[...]

    pl.when(theta_even)(lambda: polar_in(ta, tb))
    pl.when(jnp.logical_not(theta_even))(lambda: polar_in(tb, ta))
    for k in range(2 * G):
        c = [pol_u[k * z.slices + n * R : k * z.slices + (n + 1) * R, :] for n in range(6)]
        a = co[z.k_a + G : z.k_a + G + R, :]
        s = co[z.k_s + G : z.k_s + G + R, :]
        for n, value in enumerate(fields_of(c, a, s)[:4]):
            pol_e[(k * 4 + n) * R : (k * 4 + n + 1) * R, :] = value

    def theta_group(g, carry, has_e):
        base = pl.multiple_of(g * 8, 8)

        def at(ref, ghosts, per):
            def get(k):
                if G <= k < G + T:
                    return ref[pl.ds((k - G) * per + base, 8), :]
                ghost = k if k < G else k - T
                return ghosts[pl.ds(ghost * per + base, 8), :]

            return get

        def emit(j, low, high):
            acc_t[pl.ds(j * z.slices + base, 8), :] = (
                co[z.k_tp + j : z.k_tp + j + 1, :] * high
                - co[z.k_tm + j : z.k_tm + j + 1, :] * low
            )

        get_e = at(et, pol_e, 4 * R) if has_e else None
        walk(T + 1, at(ut, pol_u, z.slices), get_e, 1, emit)
        return carry

    lax.fori_loop(0, 4 * R // 8, functools.partial(theta_group, has_e=True), 0)
    lax.fori_loop(4 * R // 8, z.slices // 8, functools.partial(theta_group, has_e=False), 0)

    def rows_in(low, high):
        for c in range(6):
            span = slice(c * G * T, (c + 1) * G * T)
            rows_u[2 * c * G * T : (2 * c + 1) * G * T, :] = low[span, :]
            rows_u[(2 * c + 1) * G * T : (2 * c + 2) * G * T, :] = high[span, :]

    pl.when(row_even)(lambda: rows_in(rb, ra))
    pl.when(jnp.logical_not(row_even))(lambda: rows_in(ra, rb))
    for k in range(2 * G):
        r = k if k < G else k + R
        a = co[z.k_a + r : z.k_a + r + 1, :]
        s = co[z.k_s + r : z.k_s + r + 1, :]
        for t in range(0, T, 8):
            c = [rows_u[(2 * G * n + k) * T + t : (2 * G * n + k) * T + t + 8, :] for n in range(6)]
            values = fields_of(c, a, s)
            for n, field in enumerate(RADIAL_E):
                rows_e[(2 * G * n + k) * T + t : (2 * G * n + k) * T + t + 8, :] = values[field]

    def radial_tile(t, carry):
        base = pl.multiple_of(t * 8, 8)
        for c in range(6):
            def at(ref, ghosts, n):
                def get(k):
                    if G <= k < G + R:
                        return ref[pl.ds((n * R + k - G) * T + base, 8), :]
                    ghost = k if k < G else k - R
                    return ghosts[pl.ds((2 * G * n + ghost) * T + base, 8), :]

                return get

            spec = RADIAL[c]
            sign = spec[1] if spec else 1

            def emit(j, low, high):
                row = (c * R + j) * T + base
                across = (PHI_U.index(c) * R + j) * T + base
                inc = (
                    co[z.k_rp + j : z.k_rp + j + 1, :] * high
                    - co[z.k_rm + j : z.k_rm + j + 1, :] * low
                )
                polar = acc_t[pl.ds(base * z.slices + c * R + j, 8, stride=z.slices), :]
                rest = polar + acc_p[pl.ds(across, 8), :]
                inc = rest + inc if sign > 0 else rest - inc
                value = u_ref[pl.ds(row, 8), :] + inc
                if weight:
                    value = (1.0 - weight) * value + weight * u0_ref[pl.ds(row, 8), :]
                new[pl.ds(row, 8), :] = value

            get_e = at(e_ref, rows_e, RADIAL_E.index(spec[0])) if spec else None
            walk(R + 1, at(u_ref, rows_u, c), get_e, sign, emit)
        return carry

    lax.fori_loop(0, T // 8, radial_tile, 0)

    n = R * T

    def project(i, carry):
        row = pl.multiple_of(i * 8, 8)
        c = [new[pl.ds(k * n + row, 8), :] for k in range(6)]
        b = (c[B1], c[B2], c[B3])
        d = (c[D1], c[D2], c[D3])
        b_square = jnp.maximum(b[0] * b[0] + b[1] * b[1] + b[2] * b[2], 1.0)
        along = (b[0] * d[0] + b[1] * d[1] + b[2] * d[2]) / b_square
        d = [dk - along * bk for dk, bk in zip(d, b)]
        d_square = d[0] * d[0] + d[1] * d[1] + d[2] * d[2]
        shrink = jnp.sqrt(b_square / jnp.maximum(d_square, b_square))
        d = [dk * shrink for dk in d]
        if last:
            for k in range(3):
                m_ref[pl.ds(k * n + row, 8), :] = b[k]
                d_ref[pl.ds(k * n + row, 8), :] = d[k]
        else:
            for k, value in zip((B1, B2, B3, D1, D2, D3), (*b, *d)):
                outs[0][pl.ds(k * n + row, 8), :] = value
        return carry

    lax.fori_loop(0, n // 8, project, 0, unroll=4)
    if not last:
        prep(z, co, *outs, acc_p)


def body(mesh, magnetic, electric):
    _, R, T, L = magnetic.shape
    z = Sizes(mesh, R, T, L)
    z.check()
    n_row, n_theta, n_phi = z.n_row, z.n_theta, z.n_phi
    f32 = jnp.float32
    vmem = pl.BlockSpec(memory_space=pltpu.VMEM)
    whole = (z.slices * T, L)
    part = (4 * R * T, L)
    state_shapes = [
        whole, part, whole, part, (z.n_t, L, L),
        (6 * G * T, L), (6 * G * T, L), (G * z.slices, L), (G * z.slices, L), (2 * G, z.n_t, L),
    ]
    state_out = [jax.ShapeDtypeStruct(s, f32) for s in state_shapes]
    half_out = [jax.ShapeDtypeStruct((3 * R * T, L), f32)] * 2
    scratch = [
        pltpu.VMEM(whole, f32),
        pltpu.VMEM((z.n_u, L, L), f32),
        pltpu.VMEM(whole, f32),
        pltpu.VMEM(whole, f32),
        pltpu.VMEM((6 * 2 * G * T, L), f32),
        pltpu.VMEM((4 * 2 * G * T, L), f32),
        pltpu.VMEM((2 * G * z.slices, L), f32),
        pltpu.VMEM((2 * G * 4 * R, L), f32),
    ]
    params = pltpu.CompilerParams(vmem_limit_bytes=VMEM_LIMIT)

    row_a = [p for k in range(0, n_row - 1, 2) for p in ((k, k + 1), (k + 1, k))]
    row_b = [p for k in range(1, n_row - 1, 2) for p in ((k, k + 1), (k + 1, k))]

    def polar_pairs(odd):
        pairs = []
        for k in range(-1, n_theta):
            if k % 2 != odd:
                continue
            for p in range(n_phi):
                if k in (-1, n_theta - 1):
                    t = max(k, 0)
                    pairs.append((t * n_phi + p, t * n_phi + (p + n_phi // 2) % n_phi))
                else:
                    low, high = k * n_phi + p, (k + 1) * n_phi + p
                    pairs += [(low, high), (high, low)]
        return pairs

    def exchange(ra, rb, ta, tb, p):
        left = [(k, (k - 1) % n_phi) for k in range(n_phi)]
        right = [(k, (k + 1) % n_phi) for k in range(n_phi)]
        if n_phi == 2:
            p = lax.ppermute(p, "phi", left)
        else:
            p = jnp.concatenate(
                [lax.ppermute(p[:G], "phi", left), lax.ppermute(p[G:], "phi", right)]
            )
        return (
            lax.ppermute(ra, "row", row_a),
            lax.ppermute(rb, "row", row_b),
            lax.ppermute(ta, ("theta", "phi"), polar_pairs(1)),
            lax.ppermute(tb, ("theta", "phi"), polar_pairs(0)),
            p,
        )

    co, *state = pl.pallas_call(
        functools.partial(first_kernel, z),
        out_shape=[jax.ShapeDtypeStruct((z.k_n, L), f32)] + state_out,
        in_specs=[vmem] * 2,
        out_specs=[vmem] * 11,
        scratch_shapes=[pltpu.VMEM(part, f32)],
        compiler_params=params,
        name="first",
    )(magnetic.reshape(-1, L), electric.reshape(-1, L))
    start = state[0]
    weights = (0.0, 0.75, 1.0 / 3.0)
    for n, weight in enumerate(weights):
        last = n == len(weights) - 1
        extra = [start] if weight else []
        state = pl.pallas_call(
            functools.partial(stage_kernel, z, weight, last),
            out_shape=half_out if last else state_out,
            in_specs=[vmem] * (11 + len(extra)),
            out_specs=[vmem] * (2 if last else 10),
            scratch_shapes=scratch,
            compiler_params=params,
            name=f"stage{n}",
        )(co, *state[:5], *exchange(*state[5:]), *extra)
    return tuple(s.reshape(magnetic.shape) for s in state)


def solution(mesh):
    spec = P(None, "row", "theta", "phi")
    return jax.shard_map(
        functools.partial(body, mesh),
        mesh=mesh, in_specs=(spec, spec), out_specs=(spec, spec), check_vma=False,
    )
```
